32 devices in a mesh: dp: 1 (over z), ep: 32 (over y, x, core).
Axes of the slice: x: 4, y: 4, z: 1, core: 2. Of those that a mesh axis runs over, the one named last changes fastest.
The devices are a block of a 4x4x8 slice.
Arguments:
- x_in: bfloat16 [32768, 2048], P(('dp', 'ep'))
- norm_gain: bfloat16 [2048], replicated
- w_router: bfloat16 [2048, 64], replicated
- expert_ids: int32 [32768, 6], P(('dp', 'ep'))
- w_gate: bfloat16 [64, 2048, 1408], P('ep')
- w_up: bfloat16 [64, 2048, 1408], P('ep')
- w_down: bfloat16 [64, 1408, 2048], P('ep')
Outputs:
- output: bfloat16 [32768, 2048], P(('dp', 'ep'))
All inputs are finite; a program needn't handle non-finite values.
Results may differ from the reference program's by a relative error of at most 0.0012.
Values are sent between devices in bfloat16 or wider.
A program may use at most 768 MiB of HBM per device.

```python
import jax
import jax.numpy as jnp
from jax import lax

HIDDEN = 2048
EXPERT_FF = 1408
EXPERTS = 64
TOP_K = 6
TOKENS = 1024
GROUP_SIZE = 32

EPS = 1e-6
CAP_DEV = 2 * TOKENS * TOP_K // EXPERTS
HOT_COUNT = EXPERTS // 4
COLD_LEFT = TOKENS * TOP_K - HOT_COUNT * CAP_DEV
COLD_BASE = COLD_LEFT // (EXPERTS - HOT_COUNT)
COLD_EXTRA = COLD_LEFT % (EXPERTS - HOT_COUNT)
ROW_LIMIT = GROUP_SIZE * CAP_DEV


def draw_device(hot_flag, key):
    key_rank, key_rows, key_cols = jax.random.split(key, 3)
    expert_range = jnp.arange(EXPERTS, dtype=jnp.int32)
    noise = jax.random.randint(key_rank, (EXPERTS,), 0, EXPERTS, dtype=jnp.int32)
    score = (1 - hot_flag) * (EXPERTS * EXPERTS) + noise * EXPERTS + expert_range
    rank = jnp.argsort(jnp.argsort(score))
    counts = jnp.where(rank < HOT_COUNT, CAP_DEV, COLD_BASE + (rank - HOT_COUNT < COLD_EXTRA).astype(jnp.int32))
    bounds = jnp.cumsum(counts).astype(jnp.int32)
    flat_ids = jnp.searchsorted(bounds, jnp.arange(TOKENS * TOP_K, dtype=jnp.int32), side="right").astype(jnp.int32)
    table = flat_ids.reshape(TOP_K, TOKENS).T
    table = jax.random.permutation(key_rows, table, axis=0)
    col_score = jax.random.randint(key_cols, (TOKENS, TOP_K), 0, TOP_K, dtype=jnp.int32) * TOP_K + jnp.arange(TOP_K, dtype=jnp.int32)
    col_order = jnp.argsort(col_score, axis=1)
    return jnp.take_along_axis(table, col_order, axis=1)


def draw_routes(key):
    key_hot, key_dev = jax.random.split(key)
    hot_order = jax.random.permutation(key_hot, EXPERTS)
    hot_flag = (jnp.argsort(hot_order) < HOT_COUNT).astype(jnp.int32)
    dev_keys = jax.random.split(key_dev, GROUP_SIZE)
    routes = jax.vmap(draw_device, in_axes=(None, 0))(hot_flag, dev_keys)
    return routes.reshape(GROUP_SIZE * TOKENS, TOP_K).astype(jnp.int32)


def setup_inputs(seed: int = 0, part: int = 0) -> dict:
    shared = jax.random.split(jax.random.key(seed), 5)
    own = jax.random.split(jax.random.fold_in(jax.random.key(seed + 1), part), 2)
    x_in = (0.5 * jax.random.normal(own[0], (GROUP_SIZE * TOKENS, HIDDEN), jnp.float32)).astype(jnp.bfloat16)
    norm_gain = jax.random.uniform(shared[0], (HIDDEN,), jnp.float32, 0.5, 1.5).astype(jnp.bfloat16)
    w_router = (2.0 * HIDDEN ** -0.5 * jax.random.normal(shared[1], (HIDDEN, EXPERTS), jnp.float32)).astype(jnp.bfloat16)
    w_gate = (HIDDEN ** -0.5 * jax.random.normal(shared[2], (EXPERTS, HIDDEN, EXPERT_FF), jnp.float32)).astype(jnp.bfloat16)
    w_up = (HIDDEN ** -0.5 * jax.random.normal(shared[3], (EXPERTS, HIDDEN, EXPERT_FF), jnp.float32)).astype(jnp.bfloat16)
    w_down = (1.5 * EXPERT_FF ** -0.5 * jax.random.normal(shared[4], (EXPERTS, EXPERT_FF, HIDDEN), jnp.float32)).astype(jnp.bfloat16)
    expert_ids = draw_routes(own[1])
    return {"x_in": x_in, "norm_gain": norm_gain, "w_router": w_router, "expert_ids": expert_ids, "w_gate": w_gate, "w_up": w_up, "w_down": w_down}


def reference(x_in, norm_gain, w_router, expert_ids, w_gate, w_up, w_down):
    resid = x_in.astype(jnp.float32)
    mean_sq = jnp.mean(resid * resid, axis=-1, keepdims=True)
    normed = (resid * lax.rsqrt(mean_sq + EPS) * norm_gain.astype(jnp.float32)).astype(jnp.bfloat16)
    logits = jnp.dot(normed, w_router, preferred_element_type=jnp.float32)
    router_p = jax.nn.softmax(logits, axis=-1)
    picked = jnp.take_along_axis(router_p, expert_ids, axis=1)
    gates = picked / jnp.sum(picked, axis=1, keepdims=True)
    total = x_in.shape[0]

    def one_expert(moe_sum, inputs):
        expert, gate_w, up_w, down_w = inputs
        hits = expert_ids == expert
        weight = jnp.sum(jnp.where(hits, gates, 0.0), axis=1)
        rows = jnp.nonzero(jnp.any(hits, axis=1), size=ROW_LIMIT, fill_value=total)[0]
        sel_rows = jnp.take(normed, rows, axis=0, mode="fill", fill_value=0)
        gate_val = jnp.dot(sel_rows, gate_w, preferred_element_type=jnp.float32)
        up_val = jnp.dot(sel_rows, up_w, preferred_element_type=jnp.float32)
        hidden_act = (jax.nn.silu(gate_val) * up_val).astype(jnp.bfloat16)
        out_rows = jnp.dot(hidden_act, down_w, preferred_element_type=jnp.float32).astype(jnp.bfloat16)
        row_w = jnp.take(weight, rows, mode="fill", fill_value=0)
        moe_sum = moe_sum.at[rows].add(out_rows.astype(jnp.float32) * row_w[:, None], mode="drop")
        return moe_sum, None

    start_sum = jnp.zeros((total, HIDDEN), jnp.float32)
    moe_sum = lax.scan(one_expert, start_sum, (jnp.arange(EXPERTS, dtype=jnp.int32), w_gate, w_up, w_down))[0]
    return (resid + moe_sum).astype(jnp.bfloat16)
```

```python
import functools
import math

import jax
import jax.numpy as jnp
from jax import lax
from jax.experimental import pallas as pl
from jax.experimental.pallas import tpu as pltpu
from jax.sharding import PartitionSpec as P

EPS = 1e-6


def norm_rows(x_in, norm_gain):
    resid = x_in.astype(jnp.float32)
    mean_sq = jnp.mean(resid * resid, axis=-1, keepdims=True)
    normed = (resid * lax.rsqrt(mean_sq + EPS) * norm_gain.astype(jnp.float32)).astype(jnp.bfloat16)
    return resid, normed


def choice_weights(normed, w_router, chosen):
    logits = jnp.dot(normed, w_router, preferred_element_type=jnp.float32)
    picked = jnp.where(chosen, jax.nn.softmax(logits, axis=-1), 0.0)
    return picked / jnp.sum(picked, axis=1, keepdims=True)


def split3(value):
    hi = lax.reduce_precision(value, 8, 7)
    rest = value - hi
    mid = lax.reduce_precision(rest, 8, 7)
    low = rest - mid
    return [part.astype(jnp.bfloat16) for part in (hi, mid, low)]


def expert_mlp(rows, w_gate, w_up, w_down):
    gate_val = jnp.dot(rows, w_gate, preferred_element_type=jnp.float32)
    up_val = jnp.dot(rows, w_up, preferred_element_type=jnp.float32)
    hidden_act = (jax.nn.silu(gate_val) * up_val).astype(jnp.bfloat16)
    return jnp.dot(hidden_act, w_down, preferred_element_type=jnp.float32).astype(jnp.bfloat16)


def gather_kernel(group, own_ref, out_ref, send_sems, recv_sems, local_sem):
    side = math.isqrt(group // 2)
    tokens = own_ref.shape[0]
    half, quarter = tokens // 2, tokens // 4
    me = lax.axis_index("ep")
    core, chip = lax.rem(me, 2), me // 2
    here_x, here_y = lax.rem(chip, side), chip // side

    def device(color, a, b):
        dx, dy = (a, b) if color == 0 else (b, a)
        return (lax.rem(here_y + dy + side, side) * side + lax.rem(here_x + dx + side, side)) * 2 + core

    sibling = me + 1 - 2 * core
    barrier = pltpu.get_barrier_semaphore()
    for peer in (device(0, 1, 0), device(0, -1, 0), device(0, 0, 1), device(0, 0, -1), sibling):
        pl.semaphore_signal(barrier, inc=1, device_id={"ep": peer})
    pl.semaphore_wait(barrier, 5)

    counter = iter(range(send_sems.shape[0]))
    slots = {}

    def copy(key, src, start, rows, to, own):
        slot = slots.setdefault(key, None)
        if slot is None:
            slot = slots[key] = next(counter)
        there = out_ref.at[pl.ds(pl.multiple_of(src * tokens + start, quarter), rows)]
        return pltpu.make_async_remote_copy(
            src_ref=own_ref.at[pl.ds(start, rows)] if own else there,
            dst_ref=there,
            send_sem=send_sems.at[slot],
            recv_sem=recv_sems.at[slot],
            device_id={"ep": to},
        )

    sent, awaited = [], []

    def part(color, which):
        start = color * half
        return {"h": (start, half), "q0": (start, quarter), "q1": (start + quarter, quarter)}[which]

    def send(key, src, color, which, to, own=False):
        start, rows = part(color, which)
        dma = copy(key, src, start, rows, to, own)
        dma.start()
        sent.append(dma)

    def arrive(key, src, color, which):
        start, rows = part(color, which)
        copy(key, src, start, rows, me, False).wait_recv()
        send(("sib", *key), src, color, which, sibling)
        awaited.append((("sib", *key), color, which, src))

    colors = (0, 1)
    for color in colors:
        send(("p1", color, 1), me, color, "h", device(color, -1, 0), own=True)
        send(("p1", color, 3), me, color, "h", device(color, 1, 0), own=True)
    for color in colors:
        send(("p2", color, 0, 1), me, color, "h", device(color, 0, -1), own=True)
        send(("p2", color, 0, 3), me, color, "h", device(color, 0, 1), own=True)
    own_copy = pltpu.make_async_copy(own_ref, out_ref.at[pl.ds(pl.multiple_of(me * tokens, tokens), tokens)], local_sem)
    own_copy.start()
    own_to_sibling = copy(("own",), me, 0, tokens, sibling, True)
    own_to_sibling.start()
    sent.append(own_to_sibling)

    def second(color, a):
        src = device(color, a, 0)
        send(("p2", color, a, 1), src, color, "h", device(color, 0, -1))
        send(("p2", color, a, 3), src, color, "h", device(color, 0, 1))

    def second_arrive(color, a):
        arrive(("p2", color, a, 1), device(color, a, 1), color, "h")
        send(("p2", color, a, 2, 0), device(color, a, 1), color, "q0", device(color, 0, -1))
        arrive(("p2", color, a, 3), device(color, a, -1), color, "h")
        send(("p2", color, a, 2, 1), device(color, a, -1), color, "q1", device(color, 0, 1))

    for color in colors:
        arrive(("p1", color, 1), device(color, 1, 0), color, "h")
        send(("p1", color, 2, 0), device(color, 1, 0), color, "q0", device(color, -1, 0))
        arrive(("p1", color, 3), device(color, -1, 0), color, "h")
        send(("p1", color, 2, 1), device(color, -1, 0), color, "q1", device(color, 1, 0))
    for color in colors:
        second(color, 1)
        second(color, -1)
    for color in colors:
        second_arrive(color, 0)
    for color in colors:
        arrive(("p1", color, 2, 0), device(color, 2, 0), color, "q0")
        arrive(("p1", color, 2, 1), device(color, 2, 0), color, "q1")
        second(color, 2)
    for a in (1, -1, 2):
        for color in colors:
            second_arrive(color, a)
    for a in (0, 1, -1, 2):
        for color in colors:
            arrive(("p2", color, a, 2, 0), device(color, a, 2), color, "q0")
            arrive(("p2", color, a, 2, 1), device(color, a, 2), color, "q1")

    other = 1 - 2 * core
    for key, color, which, src in awaited:
        start, rows = part(color, which)
        copy(key, src + other, start, rows, me, False).wait_recv()
    copy(("own",), sibling, 0, tokens, me, False).wait_recv()
    for dma in sent:
        dma.wait_send()
    own_copy.wait()


def gather_rows(rows, group):
    tokens, hidden = rows.shape
    copies = 2 * (4 + 16) * 2 + 1
    return pl.pallas_call(
        functools.partial(gather_kernel, group),
        out_shape=jax.ShapeDtypeStruct((group * tokens, hidden), rows.dtype),
        in_specs=[pl.BlockSpec(memory_space=pltpu.VMEM)],
        out_specs=pl.BlockSpec(memory_space=pl.ANY),
        scratch_shapes=[pltpu.SemaphoreType.DMA((copies,)), pltpu.SemaphoreType.DMA((copies,)), pltpu.SemaphoreType.DMA],
        compiler_params=pltpu.CompilerParams(collective_id=0, has_side_effects=True),
        cost_estimate=pl.CostEstimate(flops=group * tokens * hidden * 1000, bytes_accessed=group * tokens * hidden * 4, transcendentals=0),
        name="gather_rows",
    )(rows)


def solution(mesh):
    group = mesh.shape["ep"]

    def block(x_in, norm_gain, w_router, expert_ids, w_gate, w_up, w_down):
        tokens, hidden = x_in.shape
        experts = w_router.shape[1]
        top_k = expert_ids.shape[1]
        held = w_gate.shape[0]
        capacity = 2 * tokens * top_k // experts
        slot_range = jnp.arange(capacity, dtype=jnp.int32)

        chosen = jnp.any(expert_ids[:, :, None] == jnp.arange(experts, dtype=jnp.int32), axis=1)
        place = jnp.where(chosen, jnp.cumsum(chosen.astype(jnp.int32), axis=0) - 1, -1)
        at_slot = place.T[:, None, :] == slot_range[None, :, None]
        slot_tok = jnp.sum(jnp.where(at_slot, jnp.arange(tokens, dtype=jnp.int32), 0), axis=-1)
        slot_row = slot_tok + tokens * lax.axis_index("ep")
        src_row = lax.all_to_all(slot_row.reshape(group, held, capacity), "ep", 0, 0, tiled=True)

        resid, normed = norm_rows(x_in, norm_gain)
        all_rows = gather_rows(normed, group)
        weight = choice_weights(normed, w_router, chosen)

        third = capacity // 3
        cuts = [((0, third), (third, capacity)) if e == 0 else ((0, capacity - third), (capacity - third, capacity)) for e in range(held)]
        pieces = [(e, lo, hi) for e in range(held) for lo, hi in cuts[e]]
        mixed = resid
        out_rows = None
        for k, (e, lo, hi) in enumerate(pieces):
            if k:
                src_row, out_rows = lax.optimization_barrier((src_row, out_rows))
            rows = jnp.take(all_rows, src_row[:, e, lo:hi].reshape(-1), axis=0, mode="clip")
            out_rows = expert_mlp(rows, w_gate[e], w_up[e], w_down[e])
            if k == 0:
                place, weight, _ = lax.optimization_barrier((place, weight, out_rows))
            back = lax.all_to_all(out_rows.reshape(group, hi - lo, hidden), "ep", 0, 0, tiled=True)
            back = back.reshape(group * (hi - lo), hidden)
            mix = jnp.where(
                place.reshape(tokens, group, held)[:, :, e, None] == slot_range[lo:hi],
                weight.reshape(tokens, group, held)[:, :, e, None],
                0.0,
            )
            parts = lax.optimization_barrier(split3(mix.reshape(tokens, group * (hi - lo))))
            for part in parts:
                mixed = mixed + jnp.dot(part, back, preferred_element_type=jnp.float32)
            if k < len(pieces) - 1:
                mixed = lax.optimization_barrier(mixed)
        return mixed.astype(jnp.bfloat16)

    tok_spec = P(("dp", "ep"), None)
    expert_spec = P("ep", None, None)
    return jax.shard_map(block, mesh=mesh, in_specs=(tok_spec, P(None), P(None, None), tok_spec, expert_spec, expert_spec, expert_spec), out_specs=tok_spec, check_vma=False)
```

```python
import functools
import math

import jax
import jax.numpy as jnp
from jax import lax
from jax.experimental import pallas as pl
from jax.experimental.pallas import tpu as pltpu
from jax.sharding import PartitionSpec as P

EPS = 1e-6


def norm_rows(x_in, norm_gain):
    resid = x_in.astype(jnp.float32)
    mean_sq = jnp.mean(resid * resid, axis=-1, keepdims=True)
    normed = (resid * lax.rsqrt(mean_sq + EPS) * norm_gain.astype(jnp.float32)).astype(jnp.bfloat16)
    return resid, normed


def choice_weights(normed, w_router, chosen):
    logits = jnp.dot(normed, w_router, preferred_element_type=jnp.float32)
    picked = jnp.where(chosen, jax.nn.softmax(logits, axis=-1), 0.0)
    return picked / jnp.sum(picked, axis=1, keepdims=True)


def split3(value):
    hi = lax.reduce_precision(value, 8, 7)
    rest = value - hi
    mid = lax.reduce_precision(rest, 8, 7)
    low = rest - mid
    return [part.astype(jnp.bfloat16) for part in (hi, mid, low)]


def expert_mlp(rows, w_gate, w_up, w_down):
    gate_val = jnp.dot(rows, w_gate, preferred_element_type=jnp.float32)
    up_val = jnp.dot(rows, w_up, preferred_element_type=jnp.float32)
    hidden_act = (jax.nn.silu(gate_val) * up_val).astype(jnp.bfloat16)
    return jnp.dot(hidden_act, w_down, preferred_element_type=jnp.float32).astype(jnp.bfloat16)


def gather_kernel(group, own_ref, out_ref, send_sems, recv_sems, local_sem):
    side = math.isqrt(group // 2)
    tokens = own_ref.shape[0]
    half, quarter = tokens // 2, tokens // 4
    me = lax.axis_index("ep")
    core, chip = lax.rem(me, 2), me // 2
    here_x, here_y = lax.rem(chip, side), chip // side

    def device(color, a, b):
        dx, dy = (a, b) if color == 0 else (b, a)
        return (lax.rem(here_y + dy + side, side) * side + lax.rem(here_x + dx + side, side)) * 2 + core

    sibling = me + 1 - 2 * core
    barrier = pltpu.get_barrier_semaphore()
    for peer in (device(0, 1, 0), device(0, -1, 0), device(0, 0, 1), device(0, 0, -1), sibling):
        pl.semaphore_signal(barrier, inc=1, device_id={"ep": peer})
    pl.semaphore_wait(barrier, 5)

    counter = iter(range(send_sems.shape[0]))
    slots = {}

    def copy(key, src, start, rows, to, own):
        slot = slots.setdefault(key, None)
        if slot is None:
            slot = slots[key] = next(counter)
        there = out_ref.at[pl.ds(pl.multiple_of(src * tokens + start, quarter), rows)]
        return pltpu.make_async_remote_copy(
            src_ref=own_ref.at[pl.ds(start, rows)] if own else there,
            dst_ref=there,
            send_sem=send_sems.at[slot],
            recv_sem=recv_sems.at[slot],
            device_id={"ep": to},
        )

    sent, awaited = [], []

    def part(color, which):
        start = color * half
        return {"h": (start, half), "q0": (start, quarter), "q1": (start + quarter, quarter)}[which]

    def send(key, src, color, which, to, own=False):
        start, rows = part(color, which)
        dma = copy(key, src, start, rows, to, own)
        dma.start()
        sent.append(dma)

    def arrive(key, src, color, which):
        start, rows = part(color, which)
        copy(key, src, start, rows, me, False).wait_recv()
        send(("sib", *key), src, color, which, sibling)
        awaited.append((("sib", *key), color, which, src))

    colors = (0, 1)
    for color in colors:
        send(("p1", color, 1), me, color, "h", device(color, -1, 0), own=True)
        send(("p1", color, 3), me, color, "h", device(color, 1, 0), own=True)
    for color in colors:
        send(("p2", color, 0, 1), me, color, "h", device(color, 0, -1), own=True)
        send(("p2", color, 0, 3), me, color, "h", device(color, 0, 1), own=True)
    own_copy = pltpu.make_async_copy(own_ref, out_ref.at[pl.ds(pl.multiple_of(me * tokens, tokens), tokens)], local_sem)
    own_copy.start()
    own_to_sibling = copy(("own",), me, 0, tokens, sibling, True)
    own_to_sibling.start()
    sent.append(own_to_sibling)

    def second(color, a):
        src = device(color, a, 0)
        send(("p2", color, a, 1), src, color, "h", device(color, 0, -1))
        send(("p2", color, a, 3), src, color, "h", device(color, 0, 1))

    def second_arrive(color, a):
        arrive(("p2", color, a, 1), device(color, a, 1), color, "h")
        send(("p2", color, a, 2, 0), device(color, a, 1), color, "q0", device(color, 0, -1))
        arrive(("p2", color, a, 3), device(color, a, -1), color, "h")
        send(("p2", color, a, 2, 1), device(color, a, -1), color, "q1", device(color, 0, 1))

    for color in colors:
        arrive(("p1", color, 1), device(color, 1, 0), color, "h")
        send(("p1", color, 2, 0), device(color, 1, 0), color, "q0", device(color, -1, 0))
        arrive(("p1", color, 3), device(color, -1, 0), color, "h")
        send(("p1", color, 2, 1), device(color, -1, 0), color, "q1", device(color, 1, 0))
    for color in colors:
        second(color, 1)
        second(color, -1)
    for color in colors:
        second_arrive(color, 0)
    for color in colors:
        arrive(("p1", color, 2, 0), device(color, 2, 0), color, "q0")
        arrive(("p1", color, 2, 1), device(color, 2, 0), color, "q1")
        second(color, 2)
    for a in (1, -1, 2):
        for color in colors:
            second_arrive(color, a)
    for a in (0, 1, -1, 2):
        for color in colors:
            arrive(("p2", color, a, 2, 0), device(color, a, 2), color, "q0")
            arrive(("p2", color, a, 2, 1), device(color, a, 2), color, "q1")

    other = 1 - 2 * core
    for key, color, which, src in awaited:
        start, rows = part(color, which)
        copy(key, src + other, start, rows, me, False).wait_recv()
    copy(("own",), sibling, 0, tokens, me, False).wait_recv()
    for dma in sent:
        dma.wait_send()
    own_copy.wait()


def gather_rows(rows, group):
    tokens, hidden = rows.shape
    copies = 2 * (4 + 16) * 2 + 1
    return pl.pallas_call(
        functools.partial(gather_kernel, group),
        out_shape=jax.ShapeDtypeStruct((group * tokens, hidden), rows.dtype),
        in_specs=[pl.BlockSpec(memory_space=pltpu.VMEM)],
        out_specs=pl.BlockSpec(memory_space=pl.ANY),
        scratch_shapes=[pltpu.SemaphoreType.DMA((copies,)), pltpu.SemaphoreType.DMA((copies,)), pltpu.SemaphoreType.DMA],
        compiler_params=pltpu.CompilerParams(collective_id=0, has_side_effects=True),
        cost_estimate=pl.CostEstimate(flops=group * tokens * hidden * 1000, bytes_accessed=group * tokens * hidden * 4, transcendentals=0),
        name="gather_rows",
    )(rows)


def pick_kernel(bounds, tok_ref, rows_ref, *out_refs):
    tokens, hidden = rows_ref.shape[1:]
    slots = tok_ref.shape[2]
    lanes = min(128, tokens)
    column = jnp.broadcast_to(tok_ref[0], (lanes, slots)).T
    lane = lax.broadcasted_iota(jnp.int32, (slots, lanes), 1)
    pick = jnp.concatenate([jnp.where(column == lane + start, 1.0, 0.0).astype(jnp.bfloat16) for start in range(0, tokens, lanes)], axis=1)
    width = hidden // 4
    for start in range(0, hidden, width):
        rows = jnp.dot(pick, rows_ref[0, :, start : start + width], preferred_element_type=jnp.float32).astype(jnp.bfloat16)
        for out_ref, (lo, hi) in zip(out_refs, bounds):
            out_ref[0, :, start : start + width] = rows[lo:hi]


def pick_rows(src_tok, all_rows, bounds):
    group, tokens, hidden = all_rows.shape
    slots = src_tok.shape[2]
    return pl.pallas_call(
        functools.partial(pick_kernel, bounds),
        grid=(group,),
        out_shape=[jax.ShapeDtypeStruct((group, hi - lo, hidden), all_rows.dtype) for lo, hi in bounds],
        in_specs=[pl.BlockSpec((1, 1, slots), lambda s: (s, 0, 0)), pl.BlockSpec((1, tokens, hidden), lambda s: (s, 0, 0))],
        out_specs=[pl.BlockSpec((1, hi - lo, hidden), lambda s: (s, 0, 0)) for lo, hi in bounds],
        compiler_params=pltpu.CompilerParams(vmem_limit_bytes=48 * 1024 * 1024),
        cost_estimate=pl.CostEstimate(flops=2 * group * slots * tokens * hidden, bytes_accessed=2 * group * (tokens + slots) * hidden, transcendentals=0),
        name="pick_rows",
    )(src_tok, all_rows)


def solution(mesh):
    group = mesh.shape["ep"]

    def block(x_in, norm_gain, w_router, expert_ids, w_gate, w_up, w_down):
        tokens, hidden = x_in.shape
        experts = w_router.shape[1]
        top_k = expert_ids.shape[1]
        held = w_gate.shape[0]
        capacity = 2 * tokens * top_k // experts
        slot_range = jnp.arange(capacity, dtype=jnp.int32)

        chosen = jnp.any(expert_ids[:, :, None] == jnp.arange(experts, dtype=jnp.int32), axis=1)
        earlier = jnp.arange(tokens)[:, None] >= jnp.arange(tokens)[None, :]
        count = jnp.dot(earlier.astype(jnp.bfloat16), chosen.astype(jnp.bfloat16), preferred_element_type=jnp.float32)
        place = jnp.where(chosen, count.astype(jnp.int32) - 1, -1)
        at_slot = place.T[:, None, :] == slot_range[None, :, None]
        slot_tok = jnp.sum(jnp.where(at_slot, jnp.arange(1, tokens + 1, dtype=jnp.int32), 0), axis=-1) - 1
        src_tok = lax.all_to_all(slot_tok.reshape(group, held, capacity), "ep", 0, 0, tiled=True)

        resid, normed = norm_rows(x_in, norm_gain)
        all_rows = gather_rows(normed, group).reshape(group, tokens, hidden)
        weight = choice_weights(normed, w_router, chosen)

        third = capacity // 3
        cuts = [((0, third), (third, capacity)) if e == 0 else ((0, capacity - third), (capacity - third, capacity)) for e in range(held)]
        pieces = [(e, lo, hi) for e in range(held) for lo, hi in cuts[e]]
        bounds = tuple((e * capacity + lo, e * capacity + hi) for e, lo, hi in pieces)
        piece_rows = pick_rows(src_tok.reshape(group, 1, held * capacity), all_rows, bounds)
        mixed = resid
        out_rows = None
        for k, (e, lo, hi) in enumerate(pieces):
            rows = piece_rows[k].reshape(group * (hi - lo), hidden)
            if k:
                rows, out_rows = lax.optimization_barrier((rows, out_rows))
            out_rows = expert_mlp(rows, w_gate[e], w_up[e], w_down[e])
            if k == 0:
                place, weight, _ = lax.optimization_barrier((place, weight, out_rows))
            back = lax.all_to_all(out_rows.reshape(group, hi - lo, hidden), "ep", 0, 0, tiled=True)
            back = back.reshape(group * (hi - lo), hidden)
            mix = jnp.where(
                place.reshape(tokens, group, held)[:, :, e, None] == slot_range[lo:hi],
                weight.reshape(tokens, group, held)[:, :, e, None],
                0.0,
            )
            parts = lax.optimization_barrier(split3(mix.reshape(tokens, group * (hi - lo))))
            for part in parts:
                mixed = mixed + jnp.dot(part, back, preferred_element_type=jnp.float32)
            if k < len(pieces) - 1:
                mixed = lax.optimization_barrier(mixed)
        return mixed.astype(jnp.bfloat16)

    tok_spec = P(("dp", "ep"), None)
    expert_spec = P("ep", None, None)
    return jax.shard_map(block, mesh=mesh, in_specs=(tok_spec, P(None), P(None, None), tok_spec, expert_spec, expert_spec, expert_spec), out_specs=tok_spec, check_vma=False)
```
